512 devices in a mesh: tm: 16 (over z_lo, x), chan: 32 (over z_hi, y, core).
Axes of the slice: x: 4, y: 4, z: 16 (z_hi: 4, z_lo: 4; z = z_hi * 4 + z_lo), core: 2. Of those that a mesh axis runs over, the one named last changes fastest.
Arguments:
- voltages: bfloat16 [2, 128, 2048, 1024], P(None, 'tm', 'chan'), may hold values from -6 to 6
- subspace: float32 [32, 64, 32, 1024], P('chan', 'tm'), may hold values from -0.1875 to 0.1875
- order: int32 [64], replicated, may hold values from 0 to 63, each once
- beam_seeds: int32 [256], replicated, may hold values from 1 to 65520
- flagged: int32 [16], replicated, may hold values from 0 to 511
Outputs:
- beams: bfloat16 [2, 32, 64, 512, 128], P(None, None, 'tm', 'chan')
- tracked: float32 [32, 64, 32, 1024], P('chan', 'tm')
The draws below stay inside these ranges and needn't reach their ends.
Inputs may be any that keep to these rules, and one draw needn't show every extreme that they name: `order`: each of 0 to 63 once. `flagged`: station numbers; a station may occur more than once.
All inputs are finite; a program needn't handle non-finite values.
Results may differ from the reference program's by a relative error of at most 0.0084.
Values may be sent and summed in bfloat16 or wider, within the bound.
No kernel may reach another device: no remote copies, remote signals or barrier semaphores. Data moves between devices by JAX's collectives and lax.ppermute only.
A program may use at most 64 MiB of HBM per device.

```python
import math
import jax
import jax.numpy as jnp
from jax import lax

STATIONS = 512
SIG = 1024
CH = 2048
BEAMS = 256
RANK = 32
FLAGS = 16
SUB = 2
TIME = 128
GROUPS = 32
GROUP_CH = 64


def plant(entries, rng, low, largest):
    extent = entries.shape
    place = [jax.random.randint(jax.random.fold_in(rng, axis), (), 0, extent[axis]) for axis in range(len(extent))]
    entries = entries.at[tuple(place)].set(low)
    longest = extent.index(max(extent))
    place[longest] = (place[longest] + 1) % extent[longest]
    return entries.at[tuple(place)].set(largest)


def block_levels(rng, extent, split, low, high):
    def one(position, parts):
        steps = jax.random.uniform(jax.random.fold_in(jax.random.fold_in(rng, 6), position), (parts,), jnp.float32, low / len(split), high / len(split))
        return jnp.repeat(jnp.exp(steps), extent[position] // parts).reshape((-1,) + (1,) * (len(extent) - position - 1))

    factor_of = one(*split[0])
    for cut in split[1:]:
        factor_of = factor_of * one(*cut)
    return factor_of


def centred(key, shape, scale, most, cuts=(), held_as=jnp.bfloat16):
    array = jax.random.normal(key, shape, jnp.float32) * scale
    if len(cuts) > 0:
        array = block_levels(key, shape, cuts, -0.22, 0.18) * array
    return jnp.clip(array, min=-most, max=most).astype(held_as)


def setup_inputs(seed: int = 0) -> dict:
    arg_keys = jax.random.split(jax.random.key(seed), 6)
    return {
        "voltages": centred(arg_keys[0], (SUB, TIME, CH, SIG), 1.0, 6.0, ((1, 16), (2, 32))),
        "subspace": centred(arg_keys[1], (GROUPS, GROUP_CH, RANK, SIG), SIG ** -0.5, 0.1875, ((0, 32), (1, 16)), jnp.float32),
        "order": jax.random.permutation(arg_keys[2], GROUP_CH).astype(jnp.int32),
        "beam_seeds": plant(jax.random.randint(arg_keys[3], (BEAMS,), 1, 65521), jax.random.fold_in(arg_keys[3], 1), 1, 65520).astype(jnp.int32),
        "flagged": plant(jax.random.randint(arg_keys[4], (FLAGS,), 0, STATIONS), jax.random.fold_in(arg_keys[4], 1), 0, STATIONS - 1).astype(jnp.int32),
    }


TWO_PI = 2.0 * math.pi
FULL_PRECISION = lax.Precision.HIGHEST

def beam_weights(beam_seeds, channels, stations, total_channels):
    station_no = jnp.arange(stations, dtype=jnp.int32) + 1
    delays = (station_no[:, None] * beam_seeds[None, :] % 65521).astype(jnp.float32) / 65521.0
    frequency = 1.0 + channels.astype(jnp.float32) / total_channels
    angles = delays[None, :, :] * (TWO_PI * frequency)[:, None, None]
    factor = 1.0 / math.sqrt(stations)
    cosine = jnp.cos(angles) * factor
    sine_part = jnp.sin(angles) * factor
    upper = jnp.concatenate([cosine, sine_part], axis=2)
    under = jnp.concatenate([-sine_part, cosine], axis=2)
    return jnp.concatenate([upper, under], axis=1).astype(jnp.bfloat16)

def rounded_value(values):
    narrow = lax.optimization_barrier(values.astype(jnp.bfloat16))
    return narrow.astype(jnp.float32)

def power_step(voltage_input, tracked, steering_weight):
    sample_count = voltage_input.shape[0]
    wide_product = voltage_input.astype(jnp.float32)
    steering_weight_wide = steering_weight.astype(jnp.float32)
    coarse_channel = rounded_value(tracked)
    projected_input = rounded_value(jnp.einsum('xbj,bqj->bxq', wide_product, coarse_channel, precision=FULL_PRECISION))
    beam_image = jnp.einsum('nwg,wny->ngy', projected_input, wide_product, precision=FULL_PRECISION) + sample_count * tracked
    gram = jnp.einsum('crs,cks->crk', beam_image, beam_image, precision=FULL_PRECISION)
    lower = jnp.linalg.cholesky(gram)
    tracked = jax.scipy.linalg.solve_triangular(lower, beam_image, lower=True)
    subspace_vectors = rounded_value(tracked)
    lengthwise_axis = rounded_value(jnp.einsum('xbj,bqj->bxq', wide_product, subspace_vectors, precision=FULL_PRECISION))
    mixing = rounded_value(jnp.einsum('crs,csb->crb', subspace_vectors, steering_weight_wide, precision=FULL_PRECISION))
    direct_output = jnp.einsum('edi,diy->dye', wide_product, steering_weight_wide, precision=FULL_PRECISION)
    beams = direct_output - jnp.einsum('ctr,crb->cbt', lengthwise_axis, mixing, precision=FULL_PRECISION)
    return (tracked, beams.astype(jnp.bfloat16))

def reference(voltages, subspace, order, beam_seeds, flagged):
    signals = voltages.shape[-1]
    stations = signals // 2
    per_group = order.shape[0]
    marks = jnp.any(flagged[:, None] == jnp.arange(stations, dtype=jnp.int32)[None, :], axis=0)
    keep = jnp.where(marks, 0.0, 1.0).astype(jnp.bfloat16)
    keep = jnp.concatenate([keep, keep])

    def group_work(group):
        start = (group * per_group).astype(jnp.int32)
        block = lax.dynamic_slice_in_dim(voltages, start, per_group, 2)
        block = jnp.take(block, order, axis=2) * keep
        channels = start + order.astype(jnp.int32)
        steering_weight = beam_weights(beam_seeds, channels, stations, CH)
        state = lax.dynamic_index_in_dim(subspace, group, 0, keepdims=False)
        results = []
        for part in range(SUB):
            state, formed = power_step(block[part], state, steering_weight)
            results.append(formed)
        return (jnp.stack(results), state)
    formed_all, states = lax.map(group_work, jnp.arange(GROUPS, dtype=jnp.int32))
    return (jnp.moveaxis(formed_all, 0, 1), states)
```

```python
import functools
import math

import jax
import jax.numpy as jnp
import numpy as np
from jax import lax
from jax.experimental import pallas as pl
from jax.experimental.pallas import tpu as pltpu
from jax.sharding import PartitionSpec as P

CH = 2048
SUB = 2
MIB = 1024 * 1024
TRACK_LIMIT = 48 * MIB
NT = (((1,), (1,)), ((), ()))


def half_turn_fits():
    f = 0.5 * np.cos(np.pi * (np.arange(400) + 0.5) / 400)
    square = f * f
    powers = np.stack([square**n for n in range(6)], axis=1)
    sine = np.linalg.lstsq(powers * f[:, None], np.sin(np.pi * f), rcond=None)[0]
    cosine = np.linalg.lstsq(powers, np.cos(np.pi * f), rcond=None)[0]
    return [float(v) for v in sine], [float(v) for v in cosine]


def horner(coefficients, x):
    total = jnp.full_like(x, coefficients[-1])
    for c in reversed(coefficients[:-1]):
        total = total * x + c
    return total


def select_kernel(order_any, flagged_any, x_any, out_any, *scratch):
    order_ref, flagged_ref, x_ref, pick_ref, out_ref, small_sems, in_sems, out_sems = scratch
    parts, times, per_group, signals = x_ref.shape
    owners, _, each, _ = out_any.shape
    rows = times * per_group
    stations = signals // 2
    wide = signals // in_sems.shape[1]
    cuts = [(p, c) for p in range(parts) for c in range(in_sems.shape[1])]
    small = [
        pltpu.make_async_copy(order_any, order_ref, small_sems.at[0]),
        pltpu.make_async_copy(flagged_any, flagged_ref, small_sems.at[1]),
    ]
    for copy in small:
        copy.start()
    loads = []
    for p, c in cuts:
        cut = pl.ds(c * wide, wide)
        loads.append(
            pltpu.make_async_copy(
                x_any.at[p, :, :, cut], x_ref.at[p, :, :, cut], in_sems.at[p, c]
            )
        )
        loads[-1].start()
    for copy in small:
        copy.wait()
    row = lax.broadcasted_iota(jnp.int32, (2 * times, rows), 0)
    column = lax.broadcasted_iota(jnp.int32, (2 * times, rows), 1)
    first = row < times
    base = jnp.where(first, row, row - times) * per_group
    for pair in range(per_group // 2):
        channel = jnp.where(first, order_ref[2 * pair], order_ref[2 * pair + 1])
        hit = jnp.where(column == base + channel, 1.0, 0.0)
        pick_ref[2 * times * pair : 2 * times * (pair + 1), :] = hit.astype(jnp.bfloat16)
    signal = lax.broadcasted_iota(jnp.int32, (8, signals), 1)
    station = jnp.where(signal >= stations, signal - stations, signal)
    dropped = station == flagged_ref[0]
    for entry in range(1, flagged_ref.shape[0]):
        dropped = jnp.logical_or(dropped, station == flagged_ref[entry])
    keep = jnp.where(dropped, 0.0, 1.0)
    stores = []
    for (p, c), load in zip(cuts, loads, strict=True):
        load.wait()
        cut = slice(c * wide, (c + 1) * wide)
        block = x_ref[p, :, :, cut].reshape(rows, wide)
        moved = jnp.dot(pick_ref[...], block, preferred_element_type=jnp.float32)
        moved = (moved * keep[0:1, cut]).astype(jnp.bfloat16)
        out_ref[:, p, :, cut] = moved.reshape(owners, each, wide)
        span = pl.ds(c * wide, wide)
        stores.append(
            pltpu.make_async_copy(
                out_ref.at[:, p, :, span], out_any.at[:, p, :, span], out_sems.at[p, c]
            )
        )
        stores[-1].start()
    for store in stores:
        store.wait()


def select(voltages, order, flagged, owners):
    parts, times, per_group, signals = voltages.shape
    rows = times * per_group
    cuts = 4
    hbm = pl.BlockSpec(memory_space=pltpu.HBM)
    shape = (owners, parts, rows // owners, signals)
    return pl.pallas_call(
        select_kernel,
        in_specs=[hbm] * 3,
        out_specs=hbm,
        out_shape=jax.ShapeDtypeStruct(shape, jnp.bfloat16),
        scratch_shapes=[
            pltpu.SMEM(order.shape, jnp.int32),
            pltpu.SMEM(flagged.shape, jnp.int32),
            pltpu.VMEM(voltages.shape, jnp.bfloat16),
            pltpu.VMEM((rows, rows), jnp.bfloat16),
            pltpu.VMEM(shape, jnp.bfloat16),
            pltpu.SemaphoreType.DMA((2,)),
            pltpu.SemaphoreType.DMA((parts, cuts)),
            pltpu.SemaphoreType.DMA((parts, cuts)),
        ],
        compiler_params=pltpu.CompilerParams(vmem_limit_bytes=67043328),
        cost_estimate=pl.CostEstimate(
            flops=2 * parts * rows * rows * signals,
            bytes_accessed=4 * parts * rows * signals,
            transcendentals=0,
        ),
        name="select_slots",
    )(order, flagged, voltages)


def weights_kernel(fits, channel_ref, seeds_ref, out_ref, delay_ref):
    stations, beams = delay_ref.shape
    factor = 1.0 / math.sqrt(stations)
    sine_fit, cosine_fit = fits

    @pl.when(pl.program_id(0) == 0)
    def _():
        step = 64

        def fill(block, _):
            start = pl.multiple_of(block * step, step)
            number = lax.broadcasted_iota(jnp.int32, (step, beams), 0) + (start + 1)
            product = number * seeds_ref[...]
            whole = jnp.floor(product.astype(jnp.float32) * (1.0 / 65521.0)).astype(jnp.int32)
            rest = product - whole * 65521
            rest = jnp.where(rest < 0, rest + 65521, rest)
            rest = jnp.where(rest >= 65521, rest - 65521, rest)
            delay_ref[pl.ds(start, step), :] = rest.astype(jnp.float32) / 65521.0
            return 0

        lax.fori_loop(0, stations // step, fill, 0)

    frequency = 1.0 + channel_ref[pl.program_id(0)].astype(jnp.float32) * (1.0 / CH)
    double = 2.0 * frequency
    step = 32

    def fill(block, _):
        start = pl.multiple_of(block * step, step)
        turns = delay_ref[pl.ds(start, step), :] * double
        near = jnp.floor(turns + 0.5)
        f = turns - near
        half = near * 0.5
        odd = half - jnp.floor(half)
        amplitude = factor - (4.0 * factor) * odd
        square = f * f
        real = (horner(cosine_fit, square) * amplitude).astype(jnp.bfloat16)
        imaginary = horner(sine_fit, square) * (f * amplitude)
        plus = imaginary.astype(jnp.bfloat16)
        minus = (-imaginary).astype(jnp.bfloat16)
        out_ref[pl.ds(start, step), :beams] = real
        out_ref[pl.ds(start, step), beams:] = plus
        under = pl.multiple_of(stations + start, step)
        out_ref[pl.ds(under, step), :beams] = minus
        out_ref[pl.ds(under, step), beams:] = real
        return 0

    lax.fori_loop(0, stations // step, fill, 0)


def make_weights(channels, beam_seeds, stations):
    slots = channels.shape[0]
    beams = beam_seeds.shape[0]
    return pl.pallas_call(
        functools.partial(weights_kernel, half_turn_fits()),
        grid=(slots,),
        in_specs=[
            pl.BlockSpec(memory_space=pltpu.SMEM),
            pl.BlockSpec((1, beams), lambda i: (0, 0)),
        ],
        out_specs=pl.BlockSpec((None, 2 * stations, 2 * beams), lambda i: (i, 0, 0)),
        out_shape=jax.ShapeDtypeStruct((slots, 2 * stations, 2 * beams), jnp.bfloat16),
        scratch_shapes=[pltpu.VMEM((stations, beams), jnp.float32)],
        cost_estimate=pl.CostEstimate(
            flops=slots * stations * beams * 40,
            bytes_accessed=slots * stations * beams * 8,
            transcendentals=0,
        ),
        name="steering_weights",
    )(channels, beam_seeds[None, :])


def split(values):
    high = values.astype(jnp.bfloat16)
    low = (values - high.astype(jnp.float32)).astype(jnp.bfloat16)
    return high, low


def dot(a, b, dims=(((1,), (0,)), ((), ()))):
    return lax.dot_general(a, b, dims, preferred_element_type=jnp.float32)


def inverse_factors(grams):
    rank = grams.shape[0]
    lanes = grams.shape[1]
    tall = 8
    blocks = rank // tall
    row = lax.broadcasted_iota(jnp.int32, (tall, lanes), 0)
    lane = lax.broadcasted_iota(jnp.int32, (tall, lanes), 1)
    inner = lax.rem(lane, rank)
    own = lane - inner
    pieces = [grams[tall * b : tall * (b + 1)] for b in range(blocks)]
    columns = [
        {
            b: jnp.take_along_axis(pieces[b], own + j, axis=1, mode="promise_in_bounds")
            for b in range(j // tall, blocks)
        }
        for j in range(rank)
    ]
    inverse = [jnp.where(inner == row + tall * b, 1.0, 0.0) for b in range(blocks)]
    scale = [jnp.ones((tall, lanes), jnp.float32) for _ in range(blocks)]

    def line(values, index):
        return jnp.broadcast_to(values[index : index + 1], (tall, lanes))

    for k in range(rank):
        at, inside = k // tall, k % tall
        column = columns[k]
        pivot = line(column[at], inside)
        scale[at] = jnp.where(row == inside, lax.rsqrt(pivot), scale[at])
        reciprocal = 1.0 / pivot
        factor = {b: column[b] * reciprocal for b in range(at, blocks)}
        factor[at] = jnp.where(row > inside, factor[at], 0.0)
        for j in range(k + 1, rank):
            entry = line(column[j // tall], j % tall)
            for b in range(j // tall, blocks):
                columns[j][b] = columns[j][b] - factor[b] * entry
        entry = line(inverse[at], inside)
        for b in range(at, blocks):
            inverse[b] = inverse[b] - factor[b] * entry
    return jnp.concatenate([inverse[b] * scale[b] for b in range(blocks)], axis=0)


def track_kernel(x_ref, state_ref, weight_any, beams_ref, new_ref, weight_ref, own_ref, direct_ref, sems):
    sources, parts, rows, signals = x_ref.shape
    slots, rank, _ = state_ref.shape
    times = rows // slots
    total = sources * times
    owners, _, _, mine, _ = beams_ref.shape
    images = weight_ref.shape[2]
    wide = 256
    cuts = range(0, images, wide)
    loads = []
    for j in range(slots):
        loads.append(pltpu.make_async_copy(weight_any.at[j], weight_ref.at[j], sems.at[j]))
        loads[-1].start()
    for j in range(slots):
        for part in range(parts):
            block = x_ref[:, part, times * j : times * (j + 1), :]
            own_ref[j, total * part : total * (part + 1), :] = block.reshape(total, signals)
    states = [state_ref[j] for j in range(slots)]
    vectors, shares = [], []
    for part in range(parts):
        span = slice(total * part, total * (part + 1))
        pairs, grams = [], []
        for j in range(slots):
            x = own_ref[j, span]
            y = dot(states[j].astype(jnp.bfloat16), x, NT).astype(jnp.bfloat16)
            high, low = split(dot(y, x) + float(total) * states[j])
            both = jnp.concatenate([high, low], axis=0)
            products = dot(both, both, NT)
            gram = products[:rank, :rank] + products[rank:, rank:]
            grams.append(gram + products[:rank, rank:] + products[rank:, :rank])
            pairs.append((high, low))
        if part == 0:
            for j in range(slots):
                loads[j].wait()
                for cut in cuts:
                    weight = weight_ref[j, :, cut : cut + wide]
                    direct_ref[j, :, cut : cut + wide] = dot(own_ref[j], weight)
        factors = inverse_factors(jnp.concatenate(grams, axis=1))
        for j in range(slots):
            high, low = pairs[j]
            left, under = split(factors[:, rank * j : rank * (j + 1)])
            states[j] = dot(left, high) + (dot(left, low) + dot(under, high))
        vectors.append([state.astype(jnp.bfloat16) for state in states])
        shares.append(
            [dot(own_ref[j, span], vectors[part][j], NT).astype(jnp.bfloat16) for j in range(slots)]
        )
    for j in range(slots):
        new_ref[j] = states[j]
        stack = jnp.concatenate([vectors[part][j] for part in range(parts)], axis=0)
        for cut in cuts:
            mixing = dot(stack, weight_ref[j, :, cut : cut + wide]).astype(jnp.bfloat16)
            for part in range(parts):
                removed = dot(shares[part][j], mixing[rank * part : rank * (part + 1)])
                formed = direct_ref[j, total * part : total * (part + 1), cut : cut + wide] - removed
                turned = formed.T.astype(jnp.bfloat16).reshape(wide // mine, mine, total)
                lead = cut // mine
                beams_ref[lead : lead + wide // mine, part, j] = turned


def track(x, state, weight, owners):
    slots, rank, signals = state.shape
    sources, parts, rows, _ = x.shape
    total = sources * rows // slots
    images = weight.shape[2]
    flops = 2 * parts * slots * total * signals * (images + 4 * rank)
    vmem = pl.BlockSpec(memory_space=pltpu.VMEM)
    hbm = pl.BlockSpec(memory_space=pltpu.HBM)
    beams = (owners, parts, slots, images // owners, total)
    return pl.pallas_call(
        track_kernel,
        in_specs=[vmem, vmem, hbm],
        out_specs=[vmem, vmem],
        out_shape=[
            jax.ShapeDtypeStruct(beams, jnp.bfloat16),
            jax.ShapeDtypeStruct(state.shape, jnp.float32),
        ],
        scratch_shapes=[
            pltpu.VMEM(weight.shape, jnp.bfloat16),
            pltpu.VMEM((slots, parts * total, signals), jnp.bfloat16),
            pltpu.VMEM((slots, parts * total, images), jnp.float32),
            pltpu.SemaphoreType.DMA((slots,)),
        ],
        compiler_params=pltpu.CompilerParams(vmem_limit_bytes=TRACK_LIMIT),
        cost_estimate=pl.CostEstimate(flops=flops, bytes_accessed=8 * MIB, transcendentals=0),
        name="track_and_form",
    )(x, state, weight)


def order_kernel(x_ref, out_any, sems):
    copies = []
    for part in range(out_any.shape[0]):
        copies.append(pltpu.make_async_copy(x_ref.at[:, part], out_any.at[part], sems.at[part]))
        copies[-1].start()
    for copy in copies:
        copy.wait()


def by_part(x):
    owners, parts, *rest = x.shape
    return pl.pallas_call(
        order_kernel,
        in_specs=[pl.BlockSpec(memory_space=pltpu.VMEM)],
        out_specs=pl.BlockSpec(memory_space=pltpu.HBM),
        out_shape=jax.ShapeDtypeStruct((parts, owners, *rest), x.dtype),
        scratch_shapes=[pltpu.SemaphoreType.DMA((parts,))],
        compiler_params=pltpu.CompilerParams(vmem_limit_bytes=16 * MIB),
        name="order_parts",
    )(x)


def per_device(voltages, subspace, order, beam_seeds, flagged):
    signals = voltages.shape[-1]
    slots = subspace.shape[1]
    per_group = order.shape[0]
    blocks = per_group // slots
    owners = lax.axis_size("chan")
    group = lax.axis_index("chan")
    chosen = lax.dynamic_slice_in_dim(order, lax.axis_index("tm") * slots, slots)
    channels = group * per_group + chosen
    picked = select(voltages, order, flagged, blocks)
    turned = lax.all_to_all(picked, "tm", split_axis=0, concat_axis=0, tiled=True)
    weight = make_weights(channels, beam_seeds, signals // 2)
    formed, state = track(turned, subspace[0], weight, owners)
    beams = lax.all_to_all(formed, "chan", split_axis=0, concat_axis=0, tiled=True)
    return (by_part(beams), state[None])


def solution(mesh):
    return jax.shard_map(
        per_device,
        mesh=mesh,
        in_specs=(P(None, "tm", "chan", None), P("chan", "tm", None, None), P(), P(), P()),
        out_specs=(P(None, None, "tm", "chan", None), P("chan", "tm", None, None)),
        check_vma=False,
    )
```

```python
import functools
import math

import jax
import jax.numpy as jnp
import numpy as np
from jax import lax
from jax.experimental import pallas as pl
from jax.experimental.pallas import tpu as pltpu
from jax.sharding import PartitionSpec as P

CH = 2048
SUB = 2
MIB = 1024 * 1024
TRACK_LIMIT = 48 * MIB
NT = (((1,), (1,)), ((), ()))


def half_turn_fits():
    f = 0.5 * np.cos(np.pi * (np.arange(400) + 0.5) / 400)
    square = f * f
    powers = np.stack([square**n for n in range(6)], axis=1)
    sine = np.linalg.lstsq(powers * f[:, None], np.sin(np.pi * f), rcond=None)[0]
    cosine = np.linalg.lstsq(powers, np.cos(np.pi * f), rcond=None)[0]
    return [float(v) for v in sine], [float(v) for v in cosine]


def horner(coefficients, x):
    total = jnp.full_like(x, coefficients[-1])
    for c in reversed(coefficients[:-1]):
        total = total * x + c
    return total


def select_kernel(order_any, flagged_any, x_any, out_any, *scratch):
    order_ref, flagged_ref, x_ref, pick_ref, out_ref, small_sems, in_sems, out_sems = scratch
    parts, times, per_group, signals = x_ref.shape
    owners, _, each, _ = out_any.shape
    rows = times * per_group
    stations = signals // 2
    wide = 256
    halves = out_sems.shape[1]
    small = [
        pltpu.make_async_copy(order_any, order_ref, small_sems.at[0]),
        pltpu.make_async_copy(flagged_any, flagged_ref, small_sems.at[1]),
    ]
    for copy in small:
        copy.start()
    loads = []
    for p in range(parts):
        loads.append(pltpu.make_async_copy(x_any.at[p], x_ref.at[p], in_sems.at[p]))
        loads[-1].start()
    for copy in small:
        copy.wait()
    row = lax.broadcasted_iota(jnp.int32, (2 * times, rows), 0)
    column = lax.broadcasted_iota(jnp.int32, (2 * times, rows), 1)
    first = row < times
    base = jnp.where(first, row, row - times) * per_group
    for pair in range(per_group // 2):
        channel = jnp.where(first, order_ref[2 * pair], order_ref[2 * pair + 1])
        hit = jnp.where(column == base + channel, 1.0, 0.0)
        pick_ref[2 * times * pair : 2 * times * (pair + 1), :] = hit.astype(jnp.bfloat16)
    signal = lax.broadcasted_iota(jnp.int32, (8, signals), 1)
    station = jnp.where(signal >= stations, signal - stations, signal)
    dropped = station == flagged_ref[0]
    for entry in range(1, flagged_ref.shape[0]):
        dropped = jnp.logical_or(dropped, station == flagged_ref[entry])
    keep = jnp.where(dropped, 0.0, 1.0)
    stores = []
    for p in range(parts):
        loads[p].wait()
        for h in range(halves):
            lead = pl.ds(h * owners // halves, owners // halves)
            taken = pick_ref[h * rows // halves : (h + 1) * rows // halves, :]
            for start in range(0, signals, wide):
                cut = slice(start, start + wide)
                block = x_ref[p, :, :, cut].reshape(rows, wide)
                moved = jnp.dot(taken, block, preferred_element_type=jnp.float32)
                moved = (moved * keep[0:1, cut]).astype(jnp.bfloat16)
                out_ref[lead, p, :, cut] = moved.reshape(owners // halves, each, wide)
            target = out_any.at[lead, p]
            stores.append(pltpu.make_async_copy(out_ref.at[lead, p], target, out_sems.at[p, h]))
            stores[-1].start()
    for store in stores:
        store.wait()


def select(voltages, order, flagged, owners):
    parts, times, per_group, signals = voltages.shape
    rows = times * per_group
    hbm = pl.BlockSpec(memory_space=pltpu.HBM)
    shape = (owners, parts, rows // owners, signals)
    return pl.pallas_call(
        select_kernel,
        in_specs=[hbm] * 3,
        out_specs=hbm,
        out_shape=jax.ShapeDtypeStruct(shape, jnp.bfloat16),
        scratch_shapes=[
            pltpu.SMEM(order.shape, jnp.int32),
            pltpu.SMEM(flagged.shape, jnp.int32),
            pltpu.VMEM(voltages.shape, jnp.bfloat16),
            pltpu.VMEM((rows, rows), jnp.bfloat16),
            pltpu.VMEM(shape, jnp.bfloat16),
            pltpu.SemaphoreType.DMA((2,)),
            pltpu.SemaphoreType.DMA((parts,)),
            pltpu.SemaphoreType.DMA((parts, 2)),
        ],
        compiler_params=pltpu.CompilerParams(vmem_limit_bytes=67043328),
        cost_estimate=pl.CostEstimate(
            flops=2 * parts * rows * rows * signals,
            bytes_accessed=4 * parts * rows * signals,
            transcendentals=0,
        ),
        name="select_slots",
    )(order, flagged, voltages)


def weights_kernel(fits, channel_ref, seeds_ref, out_ref, delay_ref):
    stations, beams = delay_ref.shape
    factor = 1.0 / math.sqrt(stations)
    sine_fit, cosine_fit = fits

    @pl.when(pl.program_id(0) == 0)
    def _():
        step = 64

        def fill(block, _):
            start = pl.multiple_of(block * step, step)
            number = lax.broadcasted_iota(jnp.int32, (step, beams), 0) + (start + 1)
            product = number * seeds_ref[...]
            whole = jnp.floor(product.astype(jnp.float32) * (1.0 / 65521.0)).astype(jnp.int32)
            rest = product - whole * 65521
            rest = jnp.where(rest < 0, rest + 65521, rest)
            rest = jnp.where(rest >= 65521, rest - 65521, rest)
            delay_ref[pl.ds(start, step), :] = rest.astype(jnp.float32) / 65521.0
            return 0

        lax.fori_loop(0, stations // step, fill, 0)

    frequency = 1.0 + channel_ref[pl.program_id(0)].astype(jnp.float32) * (1.0 / CH)
    double = 2.0 * frequency
    step = 32

    def fill(block, _):
        start = pl.multiple_of(block * step, step)
        turns = delay_ref[pl.ds(start, step), :] * double
        near = jnp.floor(turns + 0.5)
        f = turns - near
        half = near * 0.5
        odd = half - jnp.floor(half)
        amplitude = factor - (4.0 * factor) * odd
        square = f * f
        real = (horner(cosine_fit, square) * amplitude).astype(jnp.bfloat16)
        imaginary = horner(sine_fit, square) * (f * amplitude)
        plus = imaginary.astype(jnp.bfloat16)
        minus = (-imaginary).astype(jnp.bfloat16)
        out_ref[pl.ds(start, step), :beams] = real
        out_ref[pl.ds(start, step), beams:] = plus
        under = pl.multiple_of(stations + start, step)
        out_ref[pl.ds(under, step), :beams] = minus
        out_ref[pl.ds(under, step), beams:] = real
        return 0

    lax.fori_loop(0, stations // step, fill, 0)


def make_weights(channels, beam_seeds, stations):
    slots = channels.shape[0]
    beams = beam_seeds.shape[0]
    return pl.pallas_call(
        functools.partial(weights_kernel, half_turn_fits()),
        grid=(slots,),
        in_specs=[
            pl.BlockSpec(memory_space=pltpu.SMEM),
            pl.BlockSpec((1, beams), lambda i: (0, 0)),
        ],
        out_specs=pl.BlockSpec((None, 2 * stations, 2 * beams), lambda i: (i, 0, 0)),
        out_shape=jax.ShapeDtypeStruct((slots, 2 * stations, 2 * beams), jnp.bfloat16),
        scratch_shapes=[pltpu.VMEM((stations, beams), jnp.float32)],
        cost_estimate=pl.CostEstimate(
            flops=slots * stations * beams * 40,
            bytes_accessed=slots * stations * beams * 8,
            transcendentals=0,
        ),
        name="steering_weights",
    )(channels, beam_seeds[None, :])


def split(values):
    high = values.astype(jnp.bfloat16)
    low = (values - high.astype(jnp.float32)).astype(jnp.bfloat16)
    return high, low


def dot(a, b, dims=(((1,), (0,)), ((), ()))):
    return lax.dot_general(a, b, dims, preferred_element_type=jnp.float32)


def inverse_factors(grams):
    rank = grams.shape[0]
    lanes = grams.shape[1]
    tall = 8
    blocks = rank // tall
    row = lax.broadcasted_iota(jnp.int32, (tall, lanes), 0)
    lane = lax.broadcasted_iota(jnp.int32, (tall, lanes), 1)
    inner = lax.rem(lane, rank)
    own = lane - inner
    pieces = [grams[tall * b : tall * (b + 1)] for b in range(blocks)]
    columns = [
        {
            b: jnp.take_along_axis(pieces[b], own + j, axis=1, mode="promise_in_bounds")
            for b in range(j // tall, blocks)
        }
        for j in range(rank)
    ]
    inverse = [jnp.where(inner == row + tall * b, 1.0, 0.0) for b in range(blocks)]
    scale = [jnp.ones((tall, lanes), jnp.float32) for _ in range(blocks)]

    def line(values, index):
        return jnp.broadcast_to(values[index : index + 1], (tall, lanes))

    for k in range(rank):
        at, inside = k // tall, k % tall
        column = columns[k]
        pivot = line(column[at], inside)
        scale[at] = jnp.where(row == inside, lax.rsqrt(pivot), scale[at])
        reciprocal = 1.0 / pivot
        factor = {b: column[b] * reciprocal for b in range(at, blocks)}
        factor[at] = jnp.where(row > inside, factor[at], 0.0)
        for j in range(k + 1, rank):
            entry = line(column[j // tall], j % tall)
            for b in range(j // tall, blocks):
                columns[j][b] = columns[j][b] - factor[b] * entry
        entry = line(inverse[at], inside)
        for b in range(at, blocks):
            inverse[b] = inverse[b] - factor[b] * entry
    return jnp.concatenate([inverse[b] * scale[b] for b in range(blocks)], axis=0)


def track_kernel(x_ref, state_ref, weight_any, beams_ref, new_any, *scratch):
    weight_ref, own_ref, direct_ref, new_ref, sems, new_sem = scratch
    sources, parts, rows, signals = x_ref.shape
    slots, rank, _ = state_ref.shape
    times = rows // slots
    total = sources * times
    owners, _, _, mine, _ = beams_ref.shape
    images = weight_ref.shape[2]
    wide = 256
    cuts = range(0, images, wide)
    loads = []
    for j in range(slots):
        loads.append(pltpu.make_async_copy(weight_any.at[j], weight_ref.at[j], sems.at[j]))
    for part in range(parts):
        for j in range(part, slots, parts):
            loads[j].start()
    for j in range(slots):
        for part in range(parts):
            block = x_ref[:, part, times * j : times * (j + 1), :]
            own_ref[j, total * part : total * (part + 1), :] = block.reshape(total, signals)
    states = [state_ref[j] for j in range(slots)]
    vectors, shares = [], []
    for part in range(parts):
        span = slice(total * part, total * (part + 1))
        pairs, grams = [], []
        for j in range(slots):
            x = own_ref[j, span]
            y = dot(states[j].astype(jnp.bfloat16), x, NT).astype(jnp.bfloat16)
            high, low = split(dot(y, x) + float(total) * states[j])
            both = jnp.concatenate([high, low], axis=0)
            products = dot(both, both, NT)
            gram = products[:rank, :rank] + products[rank:, rank:]
            grams.append(gram + products[:rank, rank:] + products[rank:, :rank])
            pairs.append((high, low))
        for j in range(slots):
            if j % parts == part:
                loads[j].wait()
                for cut in cuts:
                    weight = weight_ref[j, :, cut : cut + wide]
                    direct_ref[j, :, cut : cut + wide] = dot(own_ref[j], weight)
        factors = inverse_factors(jnp.concatenate(grams, axis=1))
        for j in range(slots):
            high, low = pairs[j]
            left, under = split(factors[:, rank * j : rank * (j + 1)])
            states[j] = dot(left, high) + (dot(left, low) + dot(under, high))
            if part == parts - 1:
                new_ref[j] = states[j]
        vectors.append([state.astype(jnp.bfloat16) for state in states])
        shares.append(
            [dot(own_ref[j, span], vectors[part][j], NT).astype(jnp.bfloat16) for j in range(slots)]
        )
    leave = pltpu.make_async_copy(new_ref, new_any, new_sem)
    leave.start()
    for j in range(slots):
        stack = jnp.concatenate([vectors[part][j] for part in range(parts)], axis=0)
        for cut in cuts:
            mixing = dot(stack, weight_ref[j, :, cut : cut + wide]).astype(jnp.bfloat16)
            for part in range(parts):
                removed = dot(shares[part][j], mixing[rank * part : rank * (part + 1)])
                formed = direct_ref[j, total * part : total * (part + 1), cut : cut + wide] - removed
                turned = formed.T.astype(jnp.bfloat16).reshape(wide // mine, mine, total)
                lead = cut // mine
                beams_ref[lead : lead + wide // mine, part, j] = turned
    leave.wait()


def track(x, state, weight, owners):
    slots, rank, signals = state.shape
    sources, parts, rows, _ = x.shape
    total = sources * rows // slots
    images = weight.shape[2]
    flops = 2 * parts * slots * total * signals * (images + 4 * rank)
    vmem = pl.BlockSpec(memory_space=pltpu.VMEM)
    hbm = pl.BlockSpec(memory_space=pltpu.HBM)
    beams = (owners, parts, slots, images // owners, total)
    return pl.pallas_call(
        track_kernel,
        in_specs=[vmem, vmem, hbm],
        out_specs=[vmem, hbm],
        out_shape=[
            jax.ShapeDtypeStruct(beams, jnp.bfloat16),
            jax.ShapeDtypeStruct(state.shape, jnp.float32),
        ],
        scratch_shapes=[
            pltpu.VMEM(weight.shape, jnp.bfloat16),
            pltpu.VMEM((slots, parts * total, signals), jnp.bfloat16),
            pltpu.VMEM((slots, parts * total, images), jnp.float32),
            pltpu.VMEM(state.shape, jnp.float32),
            pltpu.SemaphoreType.DMA((slots,)),
            pltpu.SemaphoreType.DMA,
        ],
        compiler_params=pltpu.CompilerParams(vmem_limit_bytes=TRACK_LIMIT),
        cost_estimate=pl.CostEstimate(flops=flops, bytes_accessed=8 * MIB, transcendentals=0),
        name="track_and_form",
    )(x, state, weight)


def order_kernel(x_ref, out_any, sems):
    copies = []
    for part in range(out_any.shape[0]):
        copies.append(pltpu.make_async_copy(x_ref.at[:, part], out_any.at[part], sems.at[part]))
        copies[-1].start()
    for copy in copies:
        copy.wait()


def by_part(x):
    owners, parts, *rest = x.shape
    return pl.pallas_call(
        order_kernel,
        in_specs=[pl.BlockSpec(memory_space=pltpu.VMEM)],
        out_specs=pl.BlockSpec(memory_space=pltpu.HBM),
        out_shape=jax.ShapeDtypeStruct((parts, owners, *rest), x.dtype),
        scratch_shapes=[pltpu.SemaphoreType.DMA((parts,))],
        compiler_params=pltpu.CompilerParams(vmem_limit_bytes=16 * MIB),
        name="order_parts",
    )(x)


def per_device(voltages, subspace, order, beam_seeds, flagged):
    signals = voltages.shape[-1]
    slots = subspace.shape[1]
    per_group = order.shape[0]
    blocks = per_group // slots
    owners = lax.axis_size("chan")
    group = lax.axis_index("chan")
    chosen = lax.dynamic_slice_in_dim(order, lax.axis_index("tm") * slots, slots)
    channels = group * per_group + chosen
    picked = select(voltages, order, flagged, blocks)
    turned = lax.all_to_all(picked, "tm", split_axis=0, concat_axis=0, tiled=True)
    weight = make_weights(channels, beam_seeds, signals // 2)
    formed, state = track(turned, subspace[0], weight, owners)
    beams = lax.all_to_all(formed, "chan", split_axis=0, concat_axis=0, tiled=True)
    return (by_part(beams), state[None])


def solution(mesh):
    return jax.shard_map(
        per_device,
        mesh=mesh,
        in_specs=(P(None, "tm", "chan", None), P("chan", "tm", None, None), P(), P(), P()),
        out_specs=(P(None, None, "tm", "chan", None), P("chan", "tm", None, None)),
        check_vma=False,
    )
```

```python
import functools
import math

import jax
import jax.numpy as jnp
import numpy as np
from jax import lax
from jax.experimental import pallas as pl
from jax.experimental.pallas import tpu as pltpu
from jax.sharding import PartitionSpec as P

CH = 2048
SUB = 2
MIB = 1024 * 1024
TRACK_LIMIT = 48 * MIB
NT = (((1,), (1,)), ((), ()))


def half_turn_fits():
    f = 0.5 * np.cos(np.pi * (np.arange(400) + 0.5) / 400)
    square = f * f
    powers = np.stack([square**n for n in range(6)], axis=1)
    sine = np.linalg.lstsq(powers * f[:, None], np.sin(np.pi * f), rcond=None)[0]
    cosine = np.linalg.lstsq(powers, np.cos(np.pi * f), rcond=None)[0]
    return [float(v) for v in sine], [float(v) for v in cosine]


def horner(coefficients, x):
    total = jnp.full_like(x, coefficients[-1])
    for c in reversed(coefficients[:-1]):
        total = total * x + c
    return total


def select_kernel(order_any, flagged_any, x_any, out_any, *scratch):
    order_ref, flagged_ref, x_ref, pick_ref, out_ref, small_sems, in_sems, out_sems = scratch
    parts, times, per_group, signals = x_ref.shape
    owners, _, each, _ = out_any.shape
    rows = times * per_group
    stations = signals // 2
    wide = 256
    halves = out_sems.shape[1]
    small = [
        pltpu.make_async_copy(order_any, order_ref, small_sems.at[0]),
        pltpu.make_async_copy(flagged_any, flagged_ref, small_sems.at[1]),
    ]
    for copy in small:
        copy.start()
    loads = []
    for p in range(parts):
        loads.append(pltpu.make_async_copy(x_any.at[p], x_ref.at[p], in_sems.at[p]))
        loads[-1].start()
    for copy in small:
        copy.wait()
    row = lax.broadcasted_iota(jnp.int32, (2 * times, rows), 0)
    column = lax.broadcasted_iota(jnp.int32, (2 * times, rows), 1)
    first = row < times
    base = jnp.where(first, row, row - times) * per_group
    for pair in range(per_group // 2):
        channel = jnp.where(first, order_ref[2 * pair], order_ref[2 * pair + 1])
        hit = jnp.where(column == base + channel, 1.0, 0.0)
        pick_ref[2 * times * pair : 2 * times * (pair + 1), :] = hit.astype(jnp.bfloat16)
    signal = lax.broadcasted_iota(jnp.int32, (8, signals), 1)
    station = jnp.where(signal >= stations, signal - stations, signal)
    dropped = station == flagged_ref[0]
    for entry in range(1, flagged_ref.shape[0]):
        dropped = jnp.logical_or(dropped, station == flagged_ref[entry])
    keep = jnp.where(dropped, 0.0, 1.0)
    stores = []
    for p in range(parts):
        loads[p].wait()
        for h in range(halves):
            lead = pl.ds(h * owners // halves, owners // halves)
            taken = pick_ref[h * rows // halves : (h + 1) * rows // halves, :]
            for start in range(0, signals, wide):
                cut = slice(start, start + wide)
                block = x_ref[p, :, :, cut].reshape(rows, wide)
                moved = jnp.dot(taken, block, preferred_element_type=jnp.float32)
                moved = (moved * keep[0:1, cut]).astype(jnp.bfloat16)
                out_ref[lead, p, :, cut] = moved.reshape(owners // halves, each, wide)
            target = out_any.at[lead, p]
            stores.append(pltpu.make_async_copy(out_ref.at[lead, p], target, out_sems.at[p, h]))
            stores[-1].start()
    for store in stores:
        store.wait()


def select(voltages, order, flagged, owners):
    parts, times, per_group, signals = voltages.shape
    rows = times * per_group
    hbm = pl.BlockSpec(memory_space=pltpu.HBM)
    shape = (owners, parts, rows // owners, signals)
    return pl.pallas_call(
        select_kernel,
        in_specs=[hbm] * 3,
        out_specs=hbm,
        out_shape=jax.ShapeDtypeStruct(shape, jnp.bfloat16),
        scratch_shapes=[
            pltpu.SMEM(order.shape, jnp.int32),
            pltpu.SMEM(flagged.shape, jnp.int32),
            pltpu.VMEM(voltages.shape, jnp.bfloat16),
            pltpu.VMEM((rows, rows), jnp.bfloat16),
            pltpu.VMEM(shape, jnp.bfloat16),
            pltpu.SemaphoreType.DMA((2,)),
            pltpu.SemaphoreType.DMA((parts,)),
            pltpu.SemaphoreType.DMA((parts, 2)),
        ],
        compiler_params=pltpu.CompilerParams(vmem_limit_bytes=67043328),
        cost_estimate=pl.CostEstimate(
            flops=2 * parts * rows * rows * signals,
            bytes_accessed=4 * parts * rows * signals,
            transcendentals=0,
        ),
        name="select_slots",
    )(order, flagged, voltages)


def weights_kernel(fits, channel_ref, seeds_ref, out_ref, delay_ref):
    stations, beams = delay_ref.shape
    factor = 1.0 / math.sqrt(stations)
    sine_fit, cosine_fit = fits

    @pl.when(pl.program_id(0) == 0)
    def _():
        step = 64

        def fill(block, _):
            start = pl.multiple_of(block * step, step)
            number = lax.broadcasted_iota(jnp.int32, (step, beams), 0) + (start + 1)
            product = number * seeds_ref[...]
            whole = jnp.floor(product.astype(jnp.float32) * (1.0 / 65521.0)).astype(jnp.int32)
            rest = product - whole * 65521
            rest = jnp.where(rest < 0, rest + 65521, rest)
            rest = jnp.where(rest >= 65521, rest - 65521, rest)
            delay_ref[pl.ds(start, step), :] = rest.astype(jnp.float32) / 65521.0
            return 0

        lax.fori_loop(0, stations // step, fill, 0)

    frequency = 1.0 + channel_ref[pl.program_id(0)].astype(jnp.float32) * (1.0 / CH)
    double = 2.0 * frequency
    step = 32

    def fill(block, _):
        start = pl.multiple_of(block * step, step)
        turns = delay_ref[pl.ds(start, step), :] * double
        near = jnp.floor(turns + 0.5)
        f = turns - near
        half = near * 0.5
        odd = half - jnp.floor(half)
        amplitude = factor - (4.0 * factor) * odd
        square = f * f
        real = (horner(cosine_fit, square) * amplitude).astype(jnp.bfloat16)
        imaginary = horner(sine_fit, square) * (f * amplitude)
        plus = imaginary.astype(jnp.bfloat16)
        minus = (-imaginary).astype(jnp.bfloat16)
        out_ref[pl.ds(start, step), :beams] = real
        out_ref[pl.ds(start, step), beams:] = plus
        under = pl.multiple_of(stations + start, step)
        out_ref[pl.ds(under, step), :beams] = minus
        out_ref[pl.ds(under, step), beams:] = real
        return 0

    lax.fori_loop(0, stations // step, fill, 0)


def make_weights(channels, beam_seeds, stations):
    slots = channels.shape[0]
    beams = beam_seeds.shape[0]
    return pl.pallas_call(
        functools.partial(weights_kernel, half_turn_fits()),
        grid=(slots,),
        in_specs=[
            pl.BlockSpec(memory_space=pltpu.SMEM),
            pl.BlockSpec((1, beams), lambda i: (0, 0)),
        ],
        out_specs=pl.BlockSpec((None, 2 * stations, 2 * beams), lambda i: (i, 0, 0)),
        out_shape=jax.ShapeDtypeStruct((slots, 2 * stations, 2 * beams), jnp.bfloat16),
        scratch_shapes=[pltpu.VMEM((stations, beams), jnp.float32)],
        cost_estimate=pl.CostEstimate(
            flops=slots * stations * beams * 40,
            bytes_accessed=slots * stations * beams * 8,
            transcendentals=0,
        ),
        name="steering_weights",
    )(channels, beam_seeds[None, :])


def split(values):
    high = values.astype(jnp.bfloat16)
    low = (values - high.astype(jnp.float32)).astype(jnp.bfloat16)
    return high, low


def dot(a, b, dims=(((1,), (0,)), ((), ()))):
    return lax.dot_general(a, b, dims, preferred_element_type=jnp.float32)


def inverse_factors(grams):
    rank = grams.shape[0]
    lanes = grams.shape[1]
    tall = 8
    blocks = rank // tall
    row = lax.broadcasted_iota(jnp.int32, (tall, lanes), 0)
    lane = lax.broadcasted_iota(jnp.int32, (tall, lanes), 1)
    inner = lax.rem(lane, rank)
    own = lane - inner
    pieces = [grams[tall * b : tall * (b + 1)] for b in range(blocks)]
    columns = [
        {
            b: jnp.take_along_axis(pieces[b], own + j, axis=1, mode="promise_in_bounds")
            for b in range(j // tall, blocks)
        }
        for j in range(rank)
    ]
    inverse = [jnp.where(inner == row + tall * b, 1.0, 0.0) for b in range(blocks)]
    scale = [jnp.ones((tall, lanes), jnp.float32) for _ in range(blocks)]

    def line(values, index):
        return jnp.broadcast_to(values[index : index + 1], (tall, lanes))

    for k in range(rank):
        at, inside = k // tall, k % tall
        column = columns[k]
        pivot = line(column[at], inside)
        scale[at] = jnp.where(row == inside, lax.rsqrt(pivot), scale[at])
        reciprocal = 1.0 / pivot
        factor = {b: column[b] * reciprocal for b in range(at, blocks)}
        factor[at] = jnp.where(row > inside, factor[at], 0.0)
        for j in range(k + 1, rank):
            entry = line(column[j // tall], j % tall)
            for b in range(j // tall, blocks):
                columns[j][b] = columns[j][b] - factor[b] * entry
        entry = line(inverse[at], inside)
        for b in range(at, blocks):
            inverse[b] = inverse[b] - factor[b] * entry
    return jnp.concatenate([inverse[b] * scale[b] for b in range(blocks)], axis=0)


def track_kernel(x_ref, state_ref, weight_any, beams_ref, new_any, *scratch):
    weight_ref, own_ref, direct_ref, new_ref, sems, new_sem = scratch
    sources, parts, rows, signals = x_ref.shape
    slots, rank, _ = state_ref.shape
    times = rows // slots
    total = sources * times
    owners, _, _, mine, _ = beams_ref.shape
    images = weight_ref.shape[2]
    wide = 512
    cuts = range(0, images, wide)
    loads = []
    for j in range(slots):
        loads.append(pltpu.make_async_copy(weight_any.at[j], weight_ref.at[j], sems.at[j]))
    for part in range(parts):
        for j in range(part, slots, parts):
            loads[j].start()
    for j in range(slots):
        for part in range(parts):
            block = x_ref[:, part, times * j : times * (j + 1), :]
            own_ref[j, total * part : total * (part + 1), :] = block.reshape(total, signals)
    states = [state_ref[j] for j in range(slots)]
    vectors, shares = [], []
    for part in range(parts):
        span = slice(total * part, total * (part + 1))
        pairs, grams = [], []
        for j in range(slots):
            x = own_ref[j, span]
            y = dot(states[j].astype(jnp.bfloat16), x, NT).astype(jnp.bfloat16)
            high, low = split(dot(y, x) + float(total) * states[j])
            both = jnp.concatenate([high, low], axis=0)
            products = dot(both, both, NT)
            gram = products[:rank, :rank] + products[rank:, rank:]
            grams.append(gram + products[:rank, rank:] + products[rank:, :rank])
            pairs.append((high, low))
        for j in range(slots):
            if j % parts == part:
                loads[j].wait()
                for cut in cuts:
                    weight = weight_ref[j, :, cut : cut + wide]
                    direct_ref[j, :, cut : cut + wide] = dot(own_ref[j], weight)
        factors = inverse_factors(jnp.concatenate(grams, axis=1))
        for j in range(slots):
            high, low = pairs[j]
            left, under = split(factors[:, rank * j : rank * (j + 1)])
            states[j] = dot(left, high) + (dot(left, low) + dot(under, high))
            if part == parts - 1:
                new_ref[j] = states[j]
        vectors.append([state.astype(jnp.bfloat16) for state in states])
        shares.append(
            [dot(own_ref[j, span], vectors[part][j], NT).astype(jnp.bfloat16) for j in range(slots)]
        )
    leave = pltpu.make_async_copy(new_ref, new_any, new_sem)
    leave.start()
    for j in range(slots):
        stack = jnp.concatenate([vectors[part][j] for part in range(parts)], axis=0)
        for cut in cuts:
            mixing = dot(stack, weight_ref[j, :, cut : cut + wide]).astype(jnp.bfloat16)
            for part in range(parts):
                removed = dot(shares[part][j], mixing[rank * part : rank * (part + 1)])
                formed = direct_ref[j, total * part : total * (part + 1), cut : cut + wide] - removed
                turned = formed.T.astype(jnp.bfloat16).reshape(wide // mine, mine, total)
                lead = cut // mine
                beams_ref[lead : lead + wide // mine, part, j] = turned
    leave.wait()


def track(x, state, weight, owners):
    slots, rank, signals = state.shape
    sources, parts, rows, _ = x.shape
    total = sources * rows // slots
    images = weight.shape[2]
    flops = 2 * parts * slots * total * signals * (images + 4 * rank)
    vmem = pl.BlockSpec(memory_space=pltpu.VMEM)
    hbm = pl.BlockSpec(memory_space=pltpu.HBM)
    beams = (owners, parts, slots, images // owners, total)
    return pl.pallas_call(
        track_kernel,
        in_specs=[vmem, vmem, hbm],
        out_specs=[vmem, hbm],
        out_shape=[
            jax.ShapeDtypeStruct(beams, jnp.bfloat16),
            jax.ShapeDtypeStruct(state.shape, jnp.float32),
        ],
        scratch_shapes=[
            pltpu.VMEM(weight.shape, jnp.bfloat16),
            pltpu.VMEM((slots, parts * total, signals), jnp.bfloat16),
            pltpu.VMEM((slots, parts * total, images), jnp.float32),
            pltpu.VMEM(state.shape, jnp.float32),
            pltpu.SemaphoreType.DMA((slots,)),
            pltpu.SemaphoreType.DMA,
        ],
        compiler_params=pltpu.CompilerParams(vmem_limit_bytes=TRACK_LIMIT),
        cost_estimate=pl.CostEstimate(flops=flops, bytes_accessed=8 * MIB, transcendentals=0),
        name="track_and_form",
    )(x, state, weight)


def order_kernel(x_ref, out_any, sems):
    copies = []
    for part in range(out_any.shape[0]):
        copies.append(pltpu.make_async_copy(x_ref.at[:, part], out_any.at[part], sems.at[part]))
        copies[-1].start()
    for copy in copies:
        copy.wait()


def by_part(x):
    owners, parts, *rest = x.shape
    return pl.pallas_call(
        order_kernel,
        in_specs=[pl.BlockSpec(memory_space=pltpu.VMEM)],
        out_specs=pl.BlockSpec(memory_space=pltpu.HBM),
        out_shape=jax.ShapeDtypeStruct((parts, owners, *rest), x.dtype),
        scratch_shapes=[pltpu.SemaphoreType.DMA((parts,))],
        compiler_params=pltpu.CompilerParams(vmem_limit_bytes=16 * MIB),
        name="order_parts",
    )(x)


def per_device(voltages, subspace, order, beam_seeds, flagged):
    signals = voltages.shape[-1]
    slots = subspace.shape[1]
    per_group = order.shape[0]
    blocks = per_group // slots
    owners = lax.axis_size("chan")
    group = lax.axis_index("chan")
    chosen = lax.dynamic_slice_in_dim(order, lax.axis_index("tm") * slots, slots)
    channels = group * per_group + chosen
    picked = select(voltages, order, flagged, blocks)
    turned = lax.all_to_all(picked, "tm", split_axis=0, concat_axis=0, tiled=True)
    weight = make_weights(channels, beam_seeds, signals // 2)
    formed, state = track(turned, subspace[0], weight, owners)
    beams = lax.all_to_all(formed, "chan", split_axis=0, concat_axis=0, tiled=True)
    return (by_part(beams), state[None])


def solution(mesh):
    return jax.shard_map(
        per_device,
        mesh=mesh,
        in_specs=(P(None, "tm", "chan", None), P("chan", "tm", None, None), P(), P(), P()),
        out_specs=(P(None, None, "tm", "chan", None), P("chan", "tm", None, None)),
        check_vma=False,
    )
```
